64 devices in a mesh: dp: 4 (over x, y), sp: 16 (over z, core).
Axes of the slice: x: 2, y: 2, z: 8, core: 2. Of those that a mesh axis runs over, the one named last changes fastest.
The devices are a block of a 4x4x8 slice.
Arguments:
- x: bfloat16 [32768, 2048], P(('dp', 'sp')), parts along dimension 0
- gain: bfloat16 [2048], replicated
- wq: bfloat16 [2048, 2048], replicated
- wk: bfloat16 [2048, 256], replicated
- wv: bfloat16 [2048, 256], replicated
- wo: bfloat16 [2048, 2048], replicated
Outputs:
- output: bfloat16 [32768, 2048], P(('dp', 'sp')), parts along dimension 0
There are 4 independent parts. The reference program is written for one: setup_inputs(seed, part) draws one part's arguments, and reference() takes and returns one part's arrays. A program takes and returns all parts, laid end to end along the dimension named above; an argument that names none is the same for every part.
All inputs are finite; a program needn't handle non-finite values.
Results may differ from the reference program's by a relative error of at most 0.012.
Values are sent between devices in bfloat16 or wider.
A program may use at most 768 MiB of HBM per device.

```python
import jax
import jax.numpy as jnp
from jax import lax

ROWS = 8192
D = 2048
HEADS = 8
KV_HEADS = 1
HEAD = 256
THETA = 10000


def setup_inputs(seed: int = 0, part: int = 0) -> dict:
    kx, kn, kq, kk, kv, ko = jax.random.split(jax.random.key(seed), 6)

    def weights(key, rows, columns):
        return jax.random.normal(key, (rows, columns), jnp.float32) * rows**-0.5

    drawn = {
        "x": jax.random.normal(jax.random.fold_in(kx, part), (ROWS, D), jnp.float32),
        "gain": 1 + 0.1 * jax.random.normal(kn, (D,), jnp.float32),
        "wq": 2 * weights(kq, D, HEADS * HEAD),
        "wk": 2 * weights(kk, D, KV_HEADS * HEAD),
        "wv": 4 * weights(kv, D, KV_HEADS * HEAD),
        "wo": weights(ko, HEADS * HEAD, D),
    }
    return {k: v.astype(jnp.bfloat16) for k, v in drawn.items()}


def normed(x, gain):
    wide = x.astype(jnp.float32)
    scale = lax.rsqrt(jnp.mean(wide * wide, -1, keepdims=True) + 1e-6)
    return (wide * scale * gain.astype(jnp.float32)).astype(jnp.bfloat16)


def turned(t, place, theta):
    half = t.shape[-1] // 2
    angle = place.astype(jnp.float32)[:, None] * theta ** (-jnp.arange(half, dtype=jnp.float32) / half)
    cos, sin = jnp.cos(angle)[:, None], jnp.sin(angle)[:, None]
    a, b = t[..., :half].astype(jnp.float32), t[..., half:].astype(jnp.float32)
    return jnp.concatenate([a * cos - b * sin, b * cos + a * sin], -1).astype(jnp.bfloat16)


def matmul(a, w):
    return jnp.dot(a, w, preferred_element_type=jnp.float32).astype(jnp.bfloat16)


def einsum(form, a, b):
    return jnp.einsum(form, a.astype(jnp.float32), b.astype(jnp.float32))


def attention(q, k, v):
    scores = einsum("tgsd,ugd->gstu", q, k) * q.shape[-1] ** -0.5
    token = jnp.arange(q.shape[0])
    scores = jnp.where(token[:, None] >= token, scores, -jnp.inf)
    weights = jax.nn.softmax(scores, -1).astype(jnp.bfloat16)
    return einsum("gstu,ugd->tgsd", weights, v).astype(jnp.bfloat16)


def reference(x, gain, wq, wk, wv, wo):
    a, place = normed(x, gain), jnp.arange(ROWS)
    q = turned(matmul(a, wq).reshape(ROWS, HEADS, HEAD), place, THETA).reshape(ROWS, KV_HEADS, -1, HEAD)
    k = turned(matmul(a, wk).reshape(ROWS, KV_HEADS, HEAD), place, THETA)
    v = matmul(a, wv).reshape(ROWS, KV_HEADS, HEAD)
    seen = attention(q, k, v).reshape(ROWS, HEADS * HEAD)
    return (x.astype(jnp.float32) + jnp.dot(seen, wo, preferred_element_type=jnp.float32)).astype(jnp.bfloat16)
```

```python
import functools

import jax
import jax.numpy as jnp
import numpy as np
from jax import lax
from jax.experimental import pallas as pl
from jax.experimental.pallas import tpu as pltpu
from jax.sharding import PartitionSpec as P

HEAD = 256
THETA = 10000
LOG2E = 1.4426950408889634
HIDDEN = -2e30
VMEM = 63 * 2**20
MESH = pl.DeviceIdType.MESH


def _dot(a, b, ca, cb):
    return lax.dot_general(a, b, (((ca,), (cb,)), ((), ())), preferred_element_type=jnp.float32)


def _kernel(n, x_hbm, gain_hbm, wq_hbm, wk_hbm, wv_hbm, wo_hbm, table_hbm, base_hbm, y_hbm,
            x_s, a_s, gain_s, wq_s, wk_s, wv_s, wo_s, table_s, base_s, q_s, k_s, v_s, top_s, mix_s, y_s,
            load_sem, out_sem, up_send, up_recv, dn_send, dn_recv, mate_send, mate_recv):
    own, width = x_s.shape
    heads = wq_s.shape[1] // HEAD
    half = HEAD // 2
    chips = n // 2
    far = chips // 2
    me = lax.axis_index("sp")
    chip, core = me // 2, me % 2
    up, dn = lax.rem(chip + 1, chips) * 2 + core, lax.rem(chip + chips - 1, chips) * 2 + core
    mate = chip * 2 + 1 - core
    e = HEAD**-0.5 * LOG2E

    def load(i, src, dst):
        return pltpu.make_async_copy(src, dst, load_sem.at[i])

    loads = [load(0, x_hbm, x_s), load(1, gain_hbm, gain_s), load(2, wk_hbm, wk_s), load(3, wv_hbm, wv_s), load(4, table_hbm, table_s),
             load(5, base_hbm, base_s), load(6, wq_hbm, wq_s), load(7, wo_hbm, wo_s)]
    for c in loads:
        c.start()

    barrier = pltpu.get_barrier_semaphore()
    for d in (up, dn, mate):
        pl.semaphore_signal(barrier, inc=1, device_id={"sp": d}, device_id_type=MESH)

    def remote(buf, chip_of, send, recv, target):
        slot = chip_of * 2 + core
        return pltpu.make_async_remote_copy(src_ref=buf.at[slot], dst_ref=buf.at[slot], send_sem=send, recv_sem=recv,
                                            device_id={"sp": target}, device_id_type=MESH)

    def hop_up(s, kind, sending):
        block = chip - s + (1 if sending else 0)
        return remote((k_s, v_s)[kind], lax.rem(block + chips, chips), up_send.at[s - 1, kind], up_recv.at[s - 1, kind], up)

    def hop_dn(s, kind, sending):
        block = chip + s - (1 if sending else 0)
        return remote((k_s, v_s)[kind], lax.rem(block, chips), dn_send.at[s - 1, kind], dn_recv.at[s - 1, kind], dn)

    def to_mate(i, kind, block, theirs=False):
        slot = block * 2 + (1 - core if theirs else core)
        buf = (k_s, v_s)[kind]
        return pltpu.make_async_remote_copy(src_ref=buf.at[slot], dst_ref=buf.at[slot], send_sem=mate_send.at[i, kind],
                                            recv_sem=mate_recv.at[i, kind], device_id={"sp": mate}, device_id_type=MESH)

    def sends_up(s):
        return (chip >= s - 1) & (chip < chips - 1)

    def sends_dn(s):
        return lax.rem(chip + s - 1, chips) < far

    for c in loads[:2]:
        c.wait()
    gain = gain_s[...].astype(jnp.float32)
    rows = 128
    for at in range(0, own, rows):
        wide = x_s[at : at + rows, :].astype(jnp.float32)
        scale = lax.rsqrt(jnp.mean(wide * wide, -1, keepdims=True) + 1e-6)
        a_s[at : at + rows, :] = (wide * scale * gain).astype(jnp.bfloat16)
    for c in loads[2:6]:
        c.wait()
    base = base_s[pl.ds(me, 1), :]
    cos_b, sin_b = base[:, :half], base[:, half:]
    cos_t, sin_t = table_s[:, :half], table_s[:, half:]
    cos, sin = cos_b * cos_t - sin_b * sin_t, sin_b * cos_t + cos_b * sin_t
    table_s[:, :half], table_s[:, half:] = cos, sin

    def turned(t):
        t = t.astype(jnp.bfloat16).astype(jnp.float32)
        a, b = t[:, :half], t[:, half:]
        cos, sin = table_s[:, :half], table_s[:, half:]
        return jnp.concatenate([a * cos - b * sin, b * cos + a * sin], -1).astype(jnp.bfloat16)

    k_s[me] = turned(_dot(a_s[...], wk_s[...], 1, 0))
    v_s[me] = _dot(a_s[...], wv_s[...], 1, 0).astype(jnp.bfloat16).T

    pl.semaphore_wait(barrier, 3)

    @pl.when(sends_up(1))
    def _():
        for kind in (0, 1):
            hop_up(1, kind, True).start()

    @pl.when(sends_dn(1))
    def _():
        for kind in (0, 1):
            hop_dn(1, kind, True).start()

    @pl.when(core == 0)
    def _():
        for kind in (0, 1):
            to_mate(2 * far - 1, kind, chip).start()

    loads[6].wait()

    def project(h, _):
        t = _dot(a_s[...], wq_s[:, pl.ds(pl.multiple_of(h * HEAD, HEAD), HEAD)], 1, 0)
        q_s[pl.ds(pl.multiple_of(h * own, own), own), :] = turned(t)

    lax.fori_loop(0, heads, project, None)

    ones = jnp.ones((8, own), jnp.bfloat16)

    def attend(slots, masked):
        def scores(h):
            return [_dot(k_s[slot], q_s[h * own : (h + 1) * own, :], 1, 1) for slot in slots]

        def soft(h, parts):
            at = slice(h * own, (h + 1) * own)
            if masked:
                ok = lax.broadcasted_iota(jnp.int32, (own, own), 0) <= lax.broadcasted_iota(jnp.int32, (own, own), 1)
                parts = [jnp.where(ok, s, HIDDEN) for s in parts]
            top = functools.reduce(jnp.maximum, [s.max(axis=0, keepdims=True) for s in parts])
            keep = None
            if not masked:
                old = top_s[0:1, at]
                top = jnp.maximum(old, top)
                keep = jnp.exp2((old - top) * e)
            top_s[0:1, at] = top
            return [jnp.exp2((s - top) * e).astype(jnp.bfloat16) for s in parts], keep

        def mix(h, weights, keep):
            at = slice(h * own, (h + 1) * own)
            got = None
            for slot, p in zip(slots, weights):
                part = _dot(jnp.concatenate([v_s[slot], ones], axis=0), p, 1, 0)
                got = part if got is None else got + part
            mix_s[:, at] = got if keep is None else mix_s[:, at] * keep + got

        now, before = scores(0), None
        for h in range(heads):
            later = scores(h + 1) if h + 1 < heads else None
            weighed = soft(h, now)
            if before is not None:
                mix(h - 1, *before)
            before, now = weighed, later
        mix(heads - 1, *before)

    attend([me], True)

    @pl.when(core == 1)
    def _():
        for kind in (0, 1):
            to_mate(2 * far - 1, kind, chip, True).wait_recv()
        attend([mate], False)

    def pass_on(i, block, kinds):
        for kind in kinds:
            to_mate(i, kind, block).start()

    def turn(r, _):
        s, above = r // 2 + 1, lax.rem(r, 2) == 1
        last = s == far
        below_in = jnp.logical_not(above) & (chip >= s)
        block_up, block_dn = lax.rem(chip - s + chips, chips), lax.rem(chip + s, chips)
        above_in = above & (block_dn < far)
        above_used = above_in & (chip + s >= chips)

        @pl.when(below_in)
        def _():
            hop_up(s, 0, False).wait_recv()
            to_mate(r, 0, block_up).start()

            @pl.when(jnp.logical_not(last))
            def _():
                hop_up(s, 1, False).wait_recv()
                to_mate(r, 1, block_up).start()

                @pl.when(sends_up(s + 1))
                def _():
                    hop_up(s + 1, 0, True).start()

                    @pl.when(s + 1 < far)
                    def _():
                        hop_up(s + 1, 1, True).start()

            @pl.when(last)
            def _():
                hop_dn(s, 1, False).wait_recv()
                to_mate(r, 1, block_up).start()

        @pl.when(above_in)
        def _():
            for kind in (0, 1):
                hop_dn(s, kind, False).wait_recv()

            @pl.when(s + 1 < far)
            def _():
                hop_dn(s + 1, 0, True).start()

            hop_dn(s + 1, 1, True).start()

            @pl.when(above_used)
            def _():
                for kind in (0, 1):
                    to_mate(r, kind, block_dn).start()

        block = jnp.where(above, block_dn, block_up)

        @pl.when(below_in | above_used)
        def _():
            for kind in (0, 1):
                to_mate(r, kind, block, True).wait_recv()
            attend([block * 2, block * 2 + 1], False)

    lax.fori_loop(0, 2 * far - 1, turn, None)

    for h in range(heads):
        at = slice(h * own, (h + 1) * own)
        seen = mix_s[:HEAD, at] * (1 / mix_s[HEAD : HEAD + 1, at])
        a_s[:, h * HEAD : (h + 1) * HEAD] = seen.astype(jnp.bfloat16).T

    loads[7].wait()
    tile = 512

    def out(i):
        at = pl.ds(pl.multiple_of(i * tile, tile), tile)
        return pltpu.make_async_copy(y_s.at[:, at], y_hbm.at[:, at], out_sem.at[i])

    def finish(i, _):
        at = pl.ds(pl.multiple_of(i * tile, tile), tile)
        got = _dot(a_s[...], wo_s[:, at], 1, 0)
        y_s[:, at] = (x_s[:, at].astype(jnp.float32) + got).astype(jnp.bfloat16)
        out(i).start()

    lax.fori_loop(0, width // tile, finish, None)

    for s in range(1, far + 1):
        for kind in (0, 1):
            if s < far or kind == 0:
                @pl.when(sends_up(s))
                def _(s=s, kind=kind):
                    hop_up(s, kind, True).wait_send()

            if s < far or kind == 1:
                @pl.when(sends_dn(s))
                def _(s=s, kind=kind):
                    hop_dn(s, kind, True).wait_send()

    for r in range(2 * far - 1):
        s = r // 2 + 1
        used = (chip >= s) if r % 2 == 0 else (chip + s >= chips) & (lax.rem(chip + s, chips) < far)

        @pl.when(used)
        def _(r=r):
            for kind in (0, 1):
                to_mate(r, kind, 0).wait_send()

    @pl.when(core == 0)
    def _():
        for kind in (0, 1):
            to_mate(2 * far - 1, kind, chip).wait_send()

    def drain(i, _):
        out(i).wait()

    lax.fori_loop(0, width // tile, drain, None)


def solution(mesh):
    n = mesh.shape["sp"]

    def step(x, gain, wq, wk, wv, wo):
        own, width = x.shape
        half = HEAD // 2
        rate = np.float64(THETA) ** (-np.arange(half) / half)
        angle = np.arange(own)[:, None] * rate
        start = (np.arange(n) * own)[:, None] * rate
        table = jnp.asarray(np.concatenate([np.cos(angle), np.sin(angle)], -1), jnp.float32)
        base = jnp.asarray(np.concatenate([np.cos(start), np.sin(start)], -1), jnp.float32)
        heads = wq.shape[1] // HEAD
        far = n // 4
        low, wide = jnp.bfloat16, jnp.float32
        return pl.pallas_call(
            functools.partial(_kernel, n),
            out_shape=jax.ShapeDtypeStruct(x.shape, x.dtype),
            in_specs=[pl.BlockSpec(memory_space=pl.ANY)] * 8,
            out_specs=pl.BlockSpec(memory_space=pl.ANY),
            scratch_shapes=[
                pltpu.VMEM((own, width), low), pltpu.VMEM((own, width), low), pltpu.VMEM((1, width), low),
                pltpu.VMEM(wq.shape, low), pltpu.VMEM(wk.shape, low), pltpu.VMEM(wv.shape, low), pltpu.VMEM(wo.shape, low),
                pltpu.VMEM((own, HEAD), wide), pltpu.VMEM((n, HEAD), wide),
                pltpu.VMEM((heads * own, HEAD), low), pltpu.VMEM((n, own, HEAD), low), pltpu.VMEM((n, HEAD, own), low),
                pltpu.VMEM((8, heads * own), wide), pltpu.VMEM((HEAD + 8, heads * own), wide), pltpu.VMEM((own, width), low),
                pltpu.SemaphoreType.DMA((8,)), pltpu.SemaphoreType.DMA((width // 512,)),
                pltpu.SemaphoreType.DMA((far, 2)), pltpu.SemaphoreType.DMA((far, 2)),
                pltpu.SemaphoreType.DMA((far, 2)), pltpu.SemaphoreType.DMA((far, 2)),
                pltpu.SemaphoreType.DMA((2 * far, 2)), pltpu.SemaphoreType.DMA((2 * far, 2)),
            ],
            compiler_params=pltpu.CompilerParams(collective_id=0, has_side_effects=True, vmem_limit_bytes=VMEM),
            name="layer",
        )(x, gain[None], wq, wk, wv, wo, table, base)

    tokens, whole = P(("dp", "sp"), None), P(None, None)
    return jax.shard_map(step, mesh=mesh, in_specs=(tokens, P(None), whole, whole, whole, whole), out_specs=tokens, check_vma=False)
```

```python
import functools

import jax
import jax.numpy as jnp
import numpy as np
from jax import lax
from jax.experimental import pallas as pl
from jax.experimental.pallas import tpu as pltpu
from jax.sharding import PartitionSpec as P

HEAD = 256
THETA = 10000
LOG2E = 1.4426950408889634
HIDDEN = -2e30
VMEM = 60 * 2**20
PARTS = 2
ROWS = 128
TILE = 512
MESH = pl.DeviceIdType.MESH


def _dot(a, b, ca, cb):
    return lax.dot_general(a, b, (((ca,), (cb,)), ((), ())), preferred_element_type=jnp.float32)


def _kernel(n, x_hbm, gain_hbm, wq_hbm, wk_hbm, wv_hbm, wo_hbm, table_hbm, base_hbm, y_ref,
            x_s, a_s, gain_s, wq_s, wkv_s, wo_s, table_s, base_s, q_s, kv_s, top_s, mix_s,
            load_sem, x_sem, q_sem, up_send, up_recv, dn_send, dn_recv, mate_send, mate_recv):
    own, width = x_s.shape
    heads = wq_s.shape[1] // HEAD
    half = HEAD // 2
    part = own // PARTS
    chips = n // 2
    far = chips // 2
    me = lax.axis_index("sp")
    chip, core = me // 2, me % 2
    up, dn = lax.rem(chip + 1, chips) * 2 + core, lax.rem(chip + chips - 1, chips) * 2 + core
    mate = chip * 2 + 1 - core
    e = HEAD**-0.5 * LOG2E

    def load(i, src, dst):
        return pltpu.make_async_copy(src, dst, load_sem.at[i])

    def load_x(i):
        at = pl.ds(i * ROWS, ROWS)
        return pltpu.make_async_copy(x_hbm.at[at, :], x_s.at[at, :], x_sem.at[i])

    def load_q(h):
        at = pl.ds(h * HEAD, HEAD)
        return pltpu.make_async_copy(wq_hbm.at[:, at], wq_s.at[:, at], q_sem.at[h])

    loads = [load(0, gain_hbm, gain_s), load(1, wk_hbm, wkv_s.at[:, pl.ds(0, HEAD)]), load(2, wv_hbm, wkv_s.at[:, pl.ds(HEAD, HEAD)]),
             load(3, table_hbm, table_s), load(4, base_hbm, base_s), load(5, wo_hbm, wo_s)]
    loads[0].start()
    for i in range(own // ROWS):
        load_x(i).start()
    for c in loads[1:5]:
        c.start()

    barrier = pltpu.get_barrier_semaphore()
    for d in (up, dn, mate):
        pl.semaphore_signal(barrier, inc=1, device_id={"sp": d}, device_id_type=MESH)

    def remote(slot, p, send, recv, target):
        buf = kv_s.at[slot, p]
        return pltpu.make_async_remote_copy(src_ref=buf, dst_ref=buf, send_sem=send, recv_sem=recv, device_id={"sp": target},
                                            device_id_type=MESH)

    def hop_up(s, p, sending):
        block = lax.rem(chip - s + (1 if sending else 0) + chips, chips)
        return remote(block * 2 + core, p, up_send.at[s - 1, p], up_recv.at[s - 1, p], up)

    def hop_dn(s, p, sending):
        block = lax.rem(chip + s - (1 if sending else 0), chips)
        return remote(block * 2 + core, p, dn_send.at[s - 1, p], dn_recv.at[s - 1, p], dn)

    def to_mate(i, p, block, theirs=False):
        return remote(block * 2 + (1 - core if theirs else core), p, mate_send.at[i, p], mate_recv.at[i, p], mate)

    def sends_up(s):
        return (chip >= s - 1) & (chip < chips - 1)

    def sends_dn(s):
        return lax.rem(chip + s - 1, chips) < far

    def turned(t, at):
        t = t.astype(jnp.bfloat16).astype(jnp.float32)
        a, b = t[:, :half], t[:, half:]
        cos, sin = table_s[at, :half], table_s[at, half:]
        return jnp.concatenate([a * cos - b * sin, b * cos + a * sin], -1).astype(jnp.bfloat16)

    loads[0].wait()
    gain = gain_s[...].astype(jnp.float32).reshape(1, width)
    for p in range(PARTS):
        at = slice(p * part, (p + 1) * part)
        for i in range(p * part // ROWS, (p + 1) * part // ROWS):
            load_x(i).wait()
        if p == 0:
            for c in loads[3:5]:
                c.wait()
            base = base_s[pl.ds(me, 1), :]
            cos_b, sin_b = base[:, :half], base[:, half:]
            cos_t, sin_t = table_s[:, :half], table_s[:, half:]
            table_s[:, :half], table_s[:, half:] = cos_b * cos_t - sin_b * sin_t, sin_b * cos_t + cos_b * sin_t
        for i in range(p * part, (p + 1) * part, ROWS):
            wide = x_s[i : i + ROWS, :].astype(jnp.float32)
            scale = lax.rsqrt(jnp.mean(wide * wide, -1, keepdims=True) + 1e-6)
            a_s[i : i + ROWS, :] = (wide * scale * gain).astype(jnp.bfloat16)
        if p == 0:
            for c in loads[1:3]:
                c.wait()
            for h in range(heads):
                load_q(h).start()
        t = _dot(a_s[at, :], wkv_s[...], 1, 0)
        kv_s[me, p, :part, :] = turned(t[:, :HEAD], at)
        kv_s[me, p, part:, :] = t[:, HEAD:].astype(jnp.bfloat16).T
        if p == 0:
            pl.semaphore_wait(barrier, 3)

        @pl.when(sends_up(1))
        def _():
            hop_up(1, p, True).start()

        @pl.when(sends_dn(1))
        def _():
            hop_dn(1, p, True).start()

        @pl.when(core == 0)
        def _():
            to_mate(2 * far - 1, p, chip).start()

    for h in range(0, heads, 2):
        load_q(h).wait()
        load_q(h + 1).wait()
        t = _dot(a_s[...], wq_s[:, h * HEAD : (h + 2) * HEAD], 1, 0)
        for i in (0, 1):
            q_s[(h + i) * own : (h + i + 1) * own, :] = turned(t[:, i * HEAD : (i + 1) * HEAD], slice(None))
    loads[5].start()

    def attend(pieces, masked):
        ones = jnp.ones((8, part * len(pieces)), jnp.bfloat16)

        def scores(h):
            keys = jnp.concatenate([kv_s[slot, p, :part, :] for slot, p in pieces], axis=0)
            return _dot(keys, q_s[h * own : (h + 1) * own, :], 1, 1)

        def soft(h, s):
            at = slice(h * own, (h + 1) * own)
            keep = None
            if masked:
                ok = lax.broadcasted_iota(jnp.int32, s.shape, 0) <= lax.broadcasted_iota(jnp.int32, s.shape, 1)
                s = jnp.where(ok, s, HIDDEN)
                top = s.max(axis=0, keepdims=True)
            else:
                old = top_s[0:1, at]
                top = jnp.maximum(old, s.max(axis=0, keepdims=True))
                keep = jnp.exp2((old - top) * e)
            top_s[0:1, at] = top
            return jnp.exp2((s - top) * e).astype(jnp.bfloat16), keep

        def mix(h, weights, keep):
            at = slice(h * own, (h + 1) * own)
            values = jnp.concatenate([kv_s[slot, p, part:, :] for slot, p in pieces], axis=1)
            got = _dot(jnp.concatenate([values, ones], axis=0), weights, 1, 0)
            mix_s[:, at] = got if keep is None else mix_s[:, at] * keep + got

        now, before = scores(0), None
        for h in range(heads):
            later = scores(h + 1) if h + 1 < heads else None
            weighed = soft(h, now)
            if before is not None:
                mix(h - 1, *before)
            before, now = weighed, later
        mix(heads - 1, *before)

    def from_below(s):
        return chip >= s

    def from_above(s):
        return lax.rem(chip + s, chips) < far

    def used_above(s):
        return from_above(s) & (chip + s >= chips)

    def below(s):
        return lax.rem(chip - s + chips, chips)

    def above(s):
        return lax.rem(chip + s, chips)

    def first_in(s):
        @pl.when(from_below(s))
        def _():
            hop_up(s, 0, False).wait_recv()

            @pl.when((s < far) & sends_up(s + 1))
            def _():
                hop_up(s + 1, 0, True).start()

            to_mate(2 * s - 2, 0, below(s)).start()

        @pl.when((s < far) & from_above(s))
        def _():
            hop_dn(s, 0, False).wait_recv()

            @pl.when(s + 1 < far)
            def _():
                hop_dn(s + 1, 0, True).start()

            @pl.when(used_above(s))
            def _():
                to_mate(2 * s - 1, 0, above(s)).start()

    def second_in(s):
        @pl.when((s < far) & from_below(s))
        def _():
            hop_up(s, 1, False).wait_recv()

            @pl.when((s + 1 < far) & sends_up(s + 1))
            def _():
                hop_up(s + 1, 1, True).start()

            to_mate(2 * s - 2, 1, below(s)).start()

        @pl.when(from_above(s))
        def _():
            hop_dn(s, 1, False).wait_recv()

            @pl.when(s < far)
            def _():
                hop_dn(s + 1, 1, True).start()

            @pl.when((s < far) & used_above(s))
            def _():
                to_mate(2 * s - 1, 1, above(s)).start()

            @pl.when(s == far)
            def _():
                to_mate(2 * s - 2, 1, above(s)).start()

    attend([(me, p) for p in range(PARTS)], True)
    first_in(1)

    @pl.when(core == 1)
    def _():
        for p in range(PARTS):
            to_mate(2 * far - 1, p, chip, True).wait_recv()
        attend([(mate, p) for p in range(PARTS)], False)

    def early(p, _):
        @pl.when(p == 1)
        def _():
            second_in(1)

        @pl.when(from_below(1))
        def _():
            to_mate(0, p, below(1), True).wait_recv()
            attend([(below(1) * 2, p), (below(1) * 2 + 1, p)], False)

    lax.fori_loop(0, PARTS, early, None)

    def turn(r, _):
        s, odd = r // 2 + 1, lax.rem(r, 2) == 1

        @pl.when(odd)
        def _():
            first_in(s + 1)

        @pl.when(jnp.logical_not(odd))
        def _():
            second_in(s)

        block = jnp.where(odd, above(s), below(s))

        @pl.when((jnp.logical_not(odd) & from_below(s)) | (odd & used_above(s)))
        def _():
            for p in range(PARTS):
                to_mate(r, p, block, True).wait_recv()
            attend([(block * 2 + c, p) for c in (0, 1) for p in range(PARTS)], False)

    lax.fori_loop(1, 2 * far - 1, turn, None)

    for s in range(1, far + 1):
        for p in range(PARTS):
            if s < far or p == 0:
                @pl.when(sends_up(s))
                def _(s=s, p=p):
                    hop_up(s, p, True).wait_send()

            if s < far or p == 1:
                @pl.when(sends_dn(s))
                def _(s=s, p=p):
                    hop_dn(s, p, True).wait_send()

    for r in range(2 * far - 1):
        s = r // 2 + 1

        @pl.when(from_below(s) if r % 2 == 0 else used_above(s))
        def _(r=r):
            for p in range(PARTS):
                to_mate(r, p, 0).wait_send()

    @pl.when(core == 0)
    def _():
        for p in range(PARTS):
            to_mate(2 * far - 1, p, chip).wait_send()

    loads[5].wait()
    for h in range(heads):
        at = slice(h * own, (h + 1) * own)
        seen = mix_s[:HEAD, at] * (1 / mix_s[HEAD : HEAD + 1, at])
        a_s[:, h * HEAD : (h + 1) * HEAD] = seen.astype(jnp.bfloat16).T
    for i in range(0, width, TILE):
        got = _dot(a_s[...], wo_s[:, i : i + TILE], 1, 0)
        y_ref[:, i : i + TILE] = (x_s[:, i : i + TILE].astype(jnp.float32) + got).astype(jnp.bfloat16)


def solution(mesh):
    n = mesh.shape["sp"]

    def step(x, gain, wq, wk, wv, wo):
        own, width = x.shape
        half = HEAD // 2
        rate = np.float64(THETA) ** (-np.arange(half) / half)
        angle = np.arange(own)[:, None] * rate
        start = (np.arange(n) * own)[:, None] * rate
        table = jnp.asarray(np.concatenate([np.cos(angle), np.sin(angle)], -1), jnp.float32)
        base = jnp.asarray(np.concatenate([np.cos(start), np.sin(start)], -1), jnp.float32)
        heads = wq.shape[1] // HEAD
        far = n // 4
        low, wide = jnp.bfloat16, jnp.float32
        dma = pltpu.SemaphoreType.DMA
        return pl.pallas_call(
            functools.partial(_kernel, n),
            out_shape=jax.ShapeDtypeStruct(x.shape, x.dtype),
            in_specs=[pl.BlockSpec(memory_space=pl.ANY)] * 8,
            out_specs=pl.BlockSpec(memory_space=pltpu.VMEM),
            scratch_shapes=[
                pltpu.VMEM((own, width), low), pltpu.VMEM((own, width), low), pltpu.VMEM((width,), low),
                pltpu.VMEM(wq.shape, low), pltpu.VMEM((width, 2 * HEAD), low), pltpu.VMEM(wo.shape, low),
                pltpu.VMEM((own, HEAD), wide), pltpu.VMEM((n, HEAD), wide),
                pltpu.VMEM((heads * own, HEAD), low), pltpu.VMEM((n, PARTS, own // PARTS + HEAD, HEAD), low),
                pltpu.VMEM((8, heads * own), wide), pltpu.VMEM((HEAD + 8, heads * own), wide),
                dma((6,)), dma((own // ROWS,)), dma((heads,)), *[dma((far, PARTS))] * 4, *[dma((2 * far, PARTS))] * 2,
            ],
            compiler_params=pltpu.CompilerParams(collective_id=0, has_side_effects=True, vmem_limit_bytes=VMEM),
            cost_estimate=pl.CostEstimate(flops=60 * 10**9, bytes_accessed=24 * 2**20, transcendentals=0),
            name="layer",
        )(x, gain, wq, wk, wv, wo, table, base)

    tokens, whole = P(("dp", "sp"), None), P(None, None)
    return jax.shard_map(step, mesh=mesh, in_specs=(tokens, P(None), whole, whole, whole, whole), out_specs=tokens, check_vma=False)
```

```python
import functools

import jax
import jax.numpy as jnp
import numpy as np
from jax import lax
from jax.experimental import pallas as pl
from jax.experimental.pallas import tpu as pltpu
from jax.sharding import PartitionSpec as P

HEAD = 256
THETA = 10000
LOG2E = 1.4426950408889634
HIDDEN = -2e30
VMEM = 60 * 2**20
PARTS = 2
ROWS = 128
TILE = 512
MESH = pl.DeviceIdType.MESH


def _dot(a, b, ca, cb):
    return lax.dot_general(a, b, (((ca,), (cb,)), ((), ())), preferred_element_type=jnp.float32)


def _kernel(n, x_hbm, gain_hbm, wq_hbm, wk_hbm, wv_hbm, wo_hbm, table_hbm, base_hbm, y_hbm,
            x_s, a_s, gain_s, wq_s, wkv_s, wo_s, table_s, base_s, q_s, kv_s, top_s, mix_s,
            load_sem, x_sem, q_sem, out_sem, up_send, up_recv, dn_send, dn_recv, mate_send, mate_recv):
    own, width = x_s.shape
    heads = wq_s.shape[1] // HEAD
    half = HEAD // 2
    part = own // PARTS
    chips = n // 2
    far = chips // 2
    me = lax.axis_index("sp")
    chip, core = me // 2, me % 2
    up, dn = lax.rem(chip + 1, chips) * 2 + core, lax.rem(chip + chips - 1, chips) * 2 + core
    mate = chip * 2 + 1 - core
    e = HEAD**-0.5 * LOG2E

    def load(i, src, dst):
        return pltpu.make_async_copy(src, dst, load_sem.at[i])

    def load_x(i):
        at = pl.ds(i * ROWS, ROWS)
        return pltpu.make_async_copy(x_hbm.at[at, :], x_s.at[at, :], x_sem.at[i])

    def load_q(h):
        at = pl.ds(h * HEAD, HEAD)
        return pltpu.make_async_copy(wq_hbm.at[:, at], wq_s.at[:, at], q_sem.at[h])

    loads = [load(0, gain_hbm, gain_s), load(1, wk_hbm, wkv_s.at[:, pl.ds(0, HEAD)]), load(2, wv_hbm, wkv_s.at[:, pl.ds(HEAD, HEAD)]),
             load(3, table_hbm, table_s), load(4, base_hbm, base_s), load(5, wo_hbm, wo_s)]
    loads[0].start()
    for i in range(own // ROWS):
        load_x(i).start()
    for c in loads[1:5]:
        c.start()

    barrier = pltpu.get_barrier_semaphore()
    for d in (up, dn, mate):
        pl.semaphore_signal(barrier, inc=1, device_id={"sp": d}, device_id_type=MESH)

    def remote(slot, p, send, recv, target):
        buf = kv_s.at[slot, p]
        return pltpu.make_async_remote_copy(src_ref=buf, dst_ref=buf, send_sem=send, recv_sem=recv, device_id={"sp": target},
                                            device_id_type=MESH)

    def hop_up(s, p, sending):
        block = lax.rem(chip - s + (1 if sending else 0) + chips, chips)
        return remote(block * 2 + core, p, up_send.at[s - 1, p], up_recv.at[s - 1, p], up)

    def hop_dn(s, p, sending):
        block = lax.rem(chip + s - (1 if sending else 0), chips)
        return remote(block * 2 + core, p, dn_send.at[s - 1, p], dn_recv.at[s - 1, p], dn)

    def to_mate(i, p, block, theirs=False):
        return remote(block * 2 + (1 - core if theirs else core), p, mate_send.at[i, p], mate_recv.at[i, p], mate)

    def sends_up(s):
        return (chip >= s - 1) & (chip < chips - 1)

    def sends_dn(s):
        return lax.rem(chip + s - 1, chips) < far

    def turned(t, at):
        t = t.astype(jnp.bfloat16).astype(jnp.float32)
        a, b = t[:, :half], t[:, half:]
        cos, sin = table_s[at, :half], table_s[at, half:]
        return jnp.concatenate([a * cos - b * sin, b * cos + a * sin], -1).astype(jnp.bfloat16)

    loads[0].wait()
    gain = gain_s[...].astype(jnp.float32).reshape(1, width)
    for i in range(own // ROWS):
        load_x(i).wait()
        at = slice(i * ROWS, (i + 1) * ROWS)
        wide = x_s[at, :].astype(jnp.float32)
        scale = lax.rsqrt(jnp.mean(wide * wide, -1, keepdims=True) + 1e-6)
        a_s[at, :] = (wide * scale * gain).astype(jnp.bfloat16)
    for c in loads[1:5]:
        c.wait()
    for h in range(heads):
        load_q(h).start()
    base = base_s[pl.ds(me, 1), :]
    cos_b, sin_b = base[:, :half], base[:, half:]
    for p in range(PARTS):
        at = slice(p * part, (p + 1) * part)
        cos_t, sin_t = table_s[at, :half], table_s[at, half:]
        table_s[at, :half], table_s[at, half:] = cos_b * cos_t - sin_b * sin_t, sin_b * cos_t + cos_b * sin_t
        t = _dot(a_s[at, :], wkv_s[...], 1, 0)
        kv_s[me, p, :part, :] = turned(t[:, :HEAD], at)
        kv_s[me, p, part:, :] = t[:, HEAD:].astype(jnp.bfloat16).T
        if p == 0:
            pl.semaphore_wait(barrier, 3)

        @pl.when(sends_up(1))
        def _():
            hop_up(1, p, True).start()

        @pl.when(sends_dn(1))
        def _():
            hop_dn(1, p, True).start()

        @pl.when(core == 0)
        def _():
            to_mate(2 * far - 1, p, chip).start()

    for h in range(0, heads, 2):
        load_q(h).wait()
        load_q(h + 1).wait()
        t = _dot(a_s[...], wq_s[:, h * HEAD : (h + 2) * HEAD], 1, 0)
        for i in (0, 1):
            q_s[(h + i) * own : (h + i + 1) * own, :] = turned(t[:, i * HEAD : (i + 1) * HEAD], slice(None))
    loads[5].start()

    def attend(strips, first=False, hook=None):
        def scores(pieces, ranges, _):
            keys = jnp.concatenate([kv_s[slot, p, :part, :] for slot, p in pieces], axis=0)
            return _dot(keys, jnp.concatenate([q_s[at, :] for at in ranges], axis=0), 1, 1)

        def soft(strip, s):
            _, ranges, level = strip
            keep = None
            if level is not None:
                query = lax.rem(lax.broadcasted_iota(jnp.int32, s.shape, 1), s.shape[1] // len(ranges))
                s = jnp.where(lax.broadcasted_iota(jnp.int32, s.shape, 0) <= query + level, s, HIDDEN)
            top = s.max(axis=0, keepdims=True)
            if not first:
                old = jnp.concatenate([top_s[0:1, at] for at in ranges], axis=1)
                top = jnp.maximum(old, top)
                keep = jnp.exp2((old - top) * e)
            size = s.shape[1] // len(ranges)
            for i, at in enumerate(ranges):
                top_s[0:1, at] = top[:, i * size : (i + 1) * size]
            return jnp.exp2((s - top) * e).astype(jnp.bfloat16), keep

        def mix(strip, weights, keep):
            pieces, ranges, _ = strip
            values = jnp.concatenate([kv_s[slot, p, part:, :] for slot, p in pieces], axis=1)
            ones = jnp.ones((8, values.shape[1]), jnp.bfloat16)
            got = _dot(jnp.concatenate([values, ones], axis=0), weights, 1, 0)
            size = got.shape[1] // len(ranges)
            for i, at in enumerate(ranges):
                new = got[:, i * size : (i + 1) * size]
                mix_s[:, at] = new if first else mix_s[:, at] * keep[:, i * size : (i + 1) * size] + new

        now, before = scores(*strips[0]), None
        for i, strip in enumerate(strips):
            if hook is not None and i == len(strips) * 3 // 4:
                hook()
            later = scores(*strips[i + 1]) if i + 1 < len(strips) else None
            weighed = soft(strip, now)
            if before is not None:
                mix(strips[i - 1], *before)
            before, now = weighed, later
        mix(strips[-1], *before)

    def whole(pieces):
        return [(pieces, [slice(h * own, (h + 1) * own)], None) for h in range(heads)]

    def from_below(s):
        return chip >= s

    def from_above(s):
        return lax.rem(chip + s, chips) < far

    def used_above(s):
        return from_above(s) & (chip + s >= chips)

    def below(s):
        return lax.rem(chip - s + chips, chips)

    def above(s):
        return lax.rem(chip + s, chips)

    def take_up(s, p, also=True):
        @pl.when(also & from_below(s) & ((s < far) | (p == 0)))
        def _():
            hop_up(s, p, False).wait_recv()

            @pl.when((s < far) & sends_up(s + 1) & ((s + 1 < far) | (p == 0)))
            def _():
                hop_up(s + 1, p, True).start()

            to_mate(s - 1, p, below(s)).start()

    def take_dn(s, p, also=True):
        @pl.when(also & from_above(s) & ((s < far) | (p == 1)))
        def _():
            hop_dn(s, p, False).wait_recv()

            @pl.when((s < far) & ((s + 1 < far) | (p == 1)))
            def _():
                hop_dn(s + 1, p, True).start()

            @pl.when(used_above(s))
            def _():
                to_mate(jnp.where(s < far, far - 1 + s, s - 1), p, above(s)).start()

    diagonal = []
    for h in range(0, heads, 2):
        for p in range(PARTS):
            ranges = [slice((h + i) * own + p * part, (h + i) * own + (p + 1) * part) for i in (0, 1)]
            diagonal.append(([(me, i) for i in range(p + 1)], ranges, p * part))
    attend(diagonal, first=True)
    take_up(1, 0)
    take_dn(1, 0)

    def early(i, _):
        p = jnp.maximum(i - 1, 0)

        @pl.when(i == 1)
        def _():
            take_up(1, 1)
            take_dn(1, 1)

        @pl.when((i == 0) & (core == 1))
        def _():
            for q in range(PARTS):
                to_mate(2 * far - 1, q, chip, True).wait_recv()

        @pl.when((i > 0) & from_below(1))
        def _():
            to_mate(0, p, below(1), True).wait_recv()

        @pl.when(jnp.where(i == 0, core == 1, from_below(1)))
        def _():
            one = (jnp.where(i == 0, mate, below(1) * 2), p)
            two = (jnp.where(i == 0, mate, below(1) * 2 + 1), jnp.where(i == 0, 1, p))
            attend(whole([one, two]))

    lax.fori_loop(0, PARTS + 1, early, None)

    full, most = used_above(1), used_above(2)

    def turn(r, _):
        s, odd, last = r // 2 + 1, lax.rem(r, 2) == 1, r == 2 * far - 2
        lower = last | (odd & (r > 1))
        block = jnp.where(lower, below(s), above(s))
        lane = jnp.where(lower, s - 1, far - 1 + s)
        used = (lower & from_below(s)) | (jnp.logical_not(lower) & used_above(s))
        early_on, late_on = most, jnp.logical_not(most)
        within = (r == 1) | (r == 3)

        take_dn(s + 1, 0, (r == 1) | ((r == 3) & early_on))
        take_up(s + 1, 0, (r == 1) | ((r == 3) & early_on))
        take_up(s, 1, ((r == 4) & early_on) | ((r == 5) & late_on))
        take_up(far, 0, jnp.where(full, r == 5, r == 6))
        take_dn(far, 1, jnp.where(full, r == 5, r == 6))

        def hook():
            take_dn(s + 1, 0, (r == 3) & late_on)
            take_up(s + 1, 0, (r == 3) & late_on)
            take_dn(s + 1, 1)
            take_up(s + 1, 1, r == 1)

        pieces = [(block * 2 + c, p) for c in (0, 1) for p in range(PARTS)]

        @pl.when(used)
        def _():
            for p in range(PARTS):
                to_mate(lane, p, block, True).wait_recv()

        @pl.when(used & within)
        def _():
            attend(whole(pieces), hook=hook)

        @pl.when(jnp.logical_not(used) & within)
        def _():
            hook()

        @pl.when(used & jnp.logical_not(within))
        def _():
            attend(whole(pieces))

    lax.fori_loop(1, 2 * far - 1, turn, None)

    for s in range(1, far + 1):
        for p in range(PARTS):
            if s < far or p == 0:
                @pl.when(sends_up(s))
                def _(s=s, p=p):
                    hop_up(s, p, True).wait_send()

            if s < far or p == 1:
                @pl.when(sends_dn(s))
                def _(s=s, p=p):
                    hop_dn(s, p, True).wait_send()

    for i in range(2 * far - 1):
        @pl.when(from_below(i + 1) if i < far else used_above(i - far + 1))
        def _(i=i):
            for p in range(PARTS):
                to_mate(i, p, 0).wait_send()

    @pl.when(core == 0)
    def _():
        for p in range(PARTS):
            to_mate(2 * far - 1, p, chip).wait_send()

    loads[5].wait()
    for h in range(heads):
        at = slice(h * own, (h + 1) * own)
        seen = mix_s[:HEAD, at] * (1 / mix_s[HEAD : HEAD + 1, at])
        a_s[:, h * HEAD : (h + 1) * HEAD] = seen.astype(jnp.bfloat16).T
    def out(i):
        at = pl.ds(i * TILE, TILE)
        return pltpu.make_async_copy(x_s.at[:, at], y_hbm.at[:, at], out_sem.at[i])

    for i in range(width // TILE):
        at = slice(i * TILE, (i + 1) * TILE)
        got = _dot(a_s[...], wo_s[:, at], 1, 0)
        x_s[:, at] = (x_s[:, at].astype(jnp.float32) + got).astype(jnp.bfloat16)
        out(i).start()
    for i in range(width // TILE):
        out(i).wait()


def solution(mesh):
    n = mesh.shape["sp"]

    def step(x, gain, wq, wk, wv, wo):
        own, width = x.shape
        half = HEAD // 2
        rate = np.float64(THETA) ** (-np.arange(half) / half)
        angle = np.arange(own)[:, None] * rate
        start = (np.arange(n) * own)[:, None] * rate
        table = jnp.asarray(np.concatenate([np.cos(angle), np.sin(angle)], -1), jnp.float32)
        base = jnp.asarray(np.concatenate([np.cos(start), np.sin(start)], -1), jnp.float32)
        heads = wq.shape[1] // HEAD
        far = n // 4
        low, wide = jnp.bfloat16, jnp.float32
        dma = pltpu.SemaphoreType.DMA
        return pl.pallas_call(
            functools.partial(_kernel, n),
            out_shape=jax.ShapeDtypeStruct(x.shape, x.dtype),
            in_specs=[pl.BlockSpec(memory_space=pl.ANY)] * 8,
            out_specs=pl.BlockSpec(memory_space=pl.ANY),
            scratch_shapes=[
                pltpu.VMEM((own, width), low), pltpu.VMEM((own, width), low), pltpu.VMEM((width,), low),
                pltpu.VMEM(wq.shape, low), pltpu.VMEM((width, 2 * HEAD), low), pltpu.VMEM(wo.shape, low),
                pltpu.VMEM((own, HEAD), wide), pltpu.VMEM((n, HEAD), wide),
                pltpu.VMEM((heads * own, HEAD), low), pltpu.VMEM((n, PARTS, own // PARTS + HEAD, HEAD), low),
                pltpu.VMEM((8, heads * own), wide), pltpu.VMEM((HEAD + 8, heads * own), wide),
                dma((6,)), dma((own // ROWS,)), dma((heads,)), dma((width // TILE,)), *[dma((far, PARTS))] * 4, *[dma((2 * far, PARTS))] * 2,
            ],
            compiler_params=pltpu.CompilerParams(collective_id=0, has_side_effects=True, vmem_limit_bytes=VMEM),
            cost_estimate=pl.CostEstimate(flops=60 * 10**9, bytes_accessed=24 * 2**20, transcendentals=0),
            name="layer",
        )(x, gain, wq, wk, wv, wo, table, base)

    tokens, whole = P(("dp", "sp"), None), P(None, None)
    return jax.shard_map(step, mesh=mesh, in_specs=(tokens, P(None), whole, whole, whole, whole), out_specs=tokens, check_vma=False)
```

```python
import functools

import jax
import jax.numpy as jnp
import numpy as np
from jax import lax
from jax.experimental import pallas as pl
from jax.experimental.pallas import tpu as pltpu
from jax.sharding import PartitionSpec as P

HEAD = 256
THETA = 10000
LOG2E = 1.4426950408889634
HIDDEN = -2e30
VMEM = 60 * 2**20
PARTS = 2
ROWS = 128
TILE = 512
MESH = pl.DeviceIdType.MESH


def _dot(a, b, ca, cb):
    return lax.dot_general(a, b, (((ca,), (cb,)), ((), ())), preferred_element_type=jnp.float32)


def _kernel(n, x_hbm, gain_hbm, wq_hbm, wk_hbm, wv_hbm, wo_hbm, table_hbm, base_hbm, y_hbm,
            x_s, a_s, gain_s, wq_s, wkv_s, wo_s, table_s, base_s, q_s, kv_s, top_s, mix_s,
            load_sem, x_sem, q_sem, out_sem, up_send, up_recv, dn_send, dn_recv, mate_send, mate_recv):
    own, width = x_s.shape
    heads = wq_s.shape[1] // HEAD
    half = HEAD // 2
    part = own // PARTS
    chips = n // 2
    far = chips // 2
    me = lax.axis_index("sp")
    chip, core = me // 2, me % 2
    up, dn = lax.rem(chip + 1, chips) * 2 + core, lax.rem(chip + chips - 1, chips) * 2 + core
    mate = chip * 2 + 1 - core
    e = HEAD**-0.5 * LOG2E

    def load(i, src, dst):
        return pltpu.make_async_copy(src, dst, load_sem.at[i])

    def load_x(i):
        at = pl.ds(i * ROWS, ROWS)
        return pltpu.make_async_copy(x_hbm.at[at, :], x_s.at[at, :], x_sem.at[i])

    def load_q(h):
        at = pl.ds(h * HEAD, HEAD)
        return pltpu.make_async_copy(wq_hbm.at[:, at], wq_s.at[:, at], q_sem.at[h])

    loads = [load(0, gain_hbm, gain_s), load(1, wk_hbm, wkv_s.at[:, pl.ds(0, HEAD)]), load(2, wv_hbm, wkv_s.at[:, pl.ds(HEAD, HEAD)]),
             load(3, table_hbm, table_s), load(4, base_hbm, base_s), load(5, wo_hbm, wo_s)]
    loads[0].start()
    for i in range(own // ROWS):
        load_x(i).start()
    for c in loads[1:5]:
        c.start()

    barrier = pltpu.get_barrier_semaphore()
    for d in (up, dn, mate):
        pl.semaphore_signal(barrier, inc=1, device_id={"sp": d}, device_id_type=MESH)

    def remote(slot, p, send, recv, target):
        buf = kv_s.at[slot, p]
        return pltpu.make_async_remote_copy(src_ref=buf, dst_ref=buf, send_sem=send, recv_sem=recv, device_id={"sp": target},
                                            device_id_type=MESH)

    def hop_up(s, p, sending):
        block = lax.rem(chip - s + (1 if sending else 0) + chips, chips)
        return remote(block * 2 + core, p, up_send.at[s - 1, p], up_recv.at[s - 1, p], up)

    def hop_dn(s, p, sending):
        block = lax.rem(chip + s - (1 if sending else 0), chips)
        return remote(block * 2 + core, p, dn_send.at[s - 1, p], dn_recv.at[s - 1, p], dn)

    def to_mate(i, p, block, theirs=False):
        return remote(block * 2 + (1 - core if theirs else core), p, mate_send.at[i, p], mate_recv.at[i, p], mate)

    def sends_up(s):
        return (chip >= s - 1) & (chip < chips - 1)

    def sends_dn(s):
        return lax.rem(chip + s - 1, chips) < far

    def turned(t, at):
        t = t.astype(jnp.bfloat16).astype(jnp.float32)
        a, b = t[:, :half], t[:, half:]
        cos, sin = table_s[at, :half], table_s[at, half:]
        return jnp.concatenate([a * cos - b * sin, b * cos + a * sin], -1).astype(jnp.bfloat16)

    loads[0].wait()
    gain = gain_s[...].astype(jnp.float32).reshape(1, width)
    for i in range(own // ROWS):
        load_x(i).wait()
        at = slice(i * ROWS, (i + 1) * ROWS)
        wide = x_s[at, :].astype(jnp.float32)
        scale = lax.rsqrt(jnp.mean(wide * wide, -1, keepdims=True) + 1e-6)
        a_s[at, :] = (wide * scale * gain).astype(jnp.bfloat16)
    for c in loads[1:5]:
        c.wait()
    for h in range(heads):
        load_q(h).start()
    base = base_s[pl.ds(me, 1), :]
    cos_b, sin_b = base[:, :half], base[:, half:]
    for p in range(PARTS):
        at = slice(p * part, (p + 1) * part)
        cos_t, sin_t = table_s[at, :half], table_s[at, half:]
        table_s[at, :half], table_s[at, half:] = cos_b * cos_t - sin_b * sin_t, sin_b * cos_t + cos_b * sin_t
        t = _dot(a_s[at, :], wkv_s[...], 1, 0)
        kv_s[me, p, :part, :] = turned(t[:, :HEAD], at)
        kv_s[me, p, part:, :] = t[:, HEAD:].astype(jnp.bfloat16).T
        if p == 0:
            pl.semaphore_wait(barrier, 3)

        @pl.when(sends_up(1))
        def _():
            hop_up(1, p, True).start()

        @pl.when(sends_dn(1))
        def _():
            hop_dn(1, p, True).start()

        @pl.when(core == 0)
        def _():
            to_mate(2 * far - 1, p, chip).start()

    def project(h):
        load_q(h).wait()
        load_q(h + 1).wait()
        return _dot(a_s[...], wq_s[:, h * HEAD : (h + 2) * HEAD], 1, 0)

    now = project(0)
    for h in range(0, heads, 2):
        later = project(h + 2) if h + 2 < heads else None
        for i in (0, 1):
            q_s[(h + i) * own : (h + i + 1) * own, :] = turned(now[:, i * HEAD : (i + 1) * HEAD], slice(None))
        now = later
    loads[5].start()

    def attend(strips, first=False, hook=None):
        def scores(pieces, ranges, _):
            keys = jnp.concatenate([kv_s[slot, p, :part, :] for slot, p in pieces], axis=0)
            return _dot(keys, jnp.concatenate([q_s[at, :] for at in ranges], axis=0), 1, 1)

        def soft(strip, s):
            _, ranges, level = strip
            keep = None
            if level is not None:
                query = lax.rem(lax.broadcasted_iota(jnp.int32, s.shape, 1), s.shape[1] // len(ranges))
                s = jnp.where(lax.broadcasted_iota(jnp.int32, s.shape, 0) <= query + level, s, HIDDEN)
            top = s.max(axis=0, keepdims=True)
            if not first:
                old = jnp.concatenate([top_s[0:1, at] for at in ranges], axis=1)
                top = jnp.maximum(old, top)
                keep = jnp.exp2((old - top) * e)
            size = s.shape[1] // len(ranges)
            for i, at in enumerate(ranges):
                top_s[0:1, at] = top[:, i * size : (i + 1) * size]
            return jnp.exp2((s - top) * e).astype(jnp.bfloat16), keep

        def mix(strip, weights, keep):
            pieces, ranges, _ = strip
            values = jnp.concatenate([kv_s[slot, p, part:, :] for slot, p in pieces], axis=1)
            ones = jnp.ones((8, values.shape[1]), jnp.bfloat16)
            got = _dot(jnp.concatenate([values, ones], axis=0), weights, 1, 0)
            size = got.shape[1] // len(ranges)
            for i, at in enumerate(ranges):
                new = got[:, i * size : (i + 1) * size]
                mix_s[:, at] = new if first else mix_s[:, at] * keep[:, i * size : (i + 1) * size] + new

        now, before = scores(*strips[0]), None
        for i, strip in enumerate(strips):
            if hook is not None and i == len(strips) * 3 // 4:
                hook()
            later = scores(*strips[i + 1]) if i + 1 < len(strips) else None
            weighed = soft(strip, now)
            if before is not None:
                mix(strips[i - 1], *before)
            before, now = weighed, later
        mix(strips[-1], *before)

    def whole(pieces):
        return [(pieces, [slice(h * own, (h + 1) * own)], None) for h in range(heads)]

    def from_below(s):
        return chip >= s

    def from_above(s):
        return lax.rem(chip + s, chips) < far

    def used_above(s):
        return from_above(s) & (chip + s >= chips)

    def below(s):
        return lax.rem(chip - s + chips, chips)

    def above(s):
        return lax.rem(chip + s, chips)

    def take_up(s, p, also=True):
        @pl.when(also & from_below(s) & ((s < far) | (p == 0)))
        def _():
            hop_up(s, p, False).wait_recv()

            @pl.when((s < far) & sends_up(s + 1) & ((s + 1 < far) | (p == 0)))
            def _():
                hop_up(s + 1, p, True).start()

            to_mate(s - 1, p, below(s)).start()

    def take_dn(s, p, also=True):
        @pl.when(also & from_above(s) & ((s < far) | (p == 1)))
        def _():
            hop_dn(s, p, False).wait_recv()

            @pl.when((s < far) & ((s + 1 < far) | (p == 1)))
            def _():
                hop_dn(s + 1, p, True).start()

            @pl.when(used_above(s))
            def _():
                to_mate(jnp.where(s < far, far - 1 + s, s - 1), p, above(s)).start()

    diagonal = []
    for h in range(0, heads, 2):
        for p in range(PARTS):
            ranges = [slice((h + i) * own + p * part, (h + i) * own + (p + 1) * part) for i in (0, 1)]
            diagonal.append(([(me, i) for i in range(p + 1)], ranges, p * part))
    attend(diagonal, first=True)
    take_up(1, 0)
    take_dn(1, 0)

    def early(i, _):
        p = jnp.maximum(i - 1, 0)

        @pl.when(i == 2)
        def _():
            take_up(1, 1)
            take_dn(1, 1)

        @pl.when((i == 0) & (core == 1))
        def _():
            for q in range(PARTS):
                to_mate(2 * far - 1, q, chip, True).wait_recv()

        @pl.when((i > 0) & from_below(1))
        def _():
            to_mate(0, p, below(1), True).wait_recv()

        @pl.when(jnp.where(i == 0, core == 1, from_below(1)))
        def _():
            one = (jnp.where(i == 0, mate, below(1) * 2), p)
            two = (jnp.where(i == 0, mate, below(1) * 2 + 1), jnp.where(i == 0, 1, p))
            attend(whole([one, two]))

    lax.fori_loop(0, PARTS + 1, early, None)

    full, most = used_above(1), used_above(2)

    def turn(r, _):
        s, odd, last = r // 2 + 1, lax.rem(r, 2) == 1, r == 2 * far - 2
        lower = last | (odd & (r > 1))
        block = jnp.where(lower, below(s), above(s))
        lane = jnp.where(lower, s - 1, far - 1 + s)
        used = (lower & from_below(s)) | (jnp.logical_not(lower) & used_above(s))
        early_on, late_on = most, jnp.logical_not(most)
        within = (r == 1) | (r == 3)

        take_dn(s + 1, 0, (r == 1) | ((r == 3) & early_on))
        take_up(s + 1, 0, (r == 1) | ((r == 3) & early_on))
        take_up(s, 1, ((r == 4) & early_on) | ((r == 5) & late_on))
        take_up(far, 0, jnp.where(full, r == 5, r == 6))
        take_dn(far, 1, jnp.where(full, r == 5, r == 6))

        def hook():
            take_dn(s + 1, 0, (r == 3) & late_on)
            take_up(s + 1, 0, (r == 3) & late_on)
            take_dn(s + 1, 1)
            take_up(s + 1, 1, r == 1)

        pieces = [(block * 2 + c, p) for c in (0, 1) for p in range(PARTS)]

        @pl.when(used)
        def _():
            for p in range(PARTS):
                to_mate(lane, p, block, True).wait_recv()

        @pl.when(used & within)
        def _():
            attend(whole(pieces), hook=hook)

        @pl.when(jnp.logical_not(used) & within)
        def _():
            hook()

        @pl.when(used & jnp.logical_not(within))
        def _():
            attend(whole(pieces))

    lax.fori_loop(1, 2 * far - 1, turn, None)

    for s in range(1, far + 1):
        for p in range(PARTS):
            if s < far or p == 0:
                @pl.when(sends_up(s))
                def _(s=s, p=p):
                    hop_up(s, p, True).wait_send()

            if s < far or p == 1:
                @pl.when(sends_dn(s))
                def _(s=s, p=p):
                    hop_dn(s, p, True).wait_send()

    for i in range(2 * far - 1):
        @pl.when(from_below(i + 1) if i < far else used_above(i - far + 1))
        def _(i=i):
            for p in range(PARTS):
                to_mate(i, p, 0).wait_send()

    @pl.when(core == 0)
    def _():
        for p in range(PARTS):
            to_mate(2 * far - 1, p, chip).wait_send()

    loads[5].wait()
    for h in range(heads):
        at = slice(h * own, (h + 1) * own)
        seen = mix_s[:HEAD, at] * (1 / mix_s[HEAD : HEAD + 1, at])
        a_s[:, h * HEAD : (h + 1) * HEAD] = seen.astype(jnp.bfloat16).T
    def out(i):
        at = pl.ds(i * TILE, TILE)
        return pltpu.make_async_copy(x_s.at[:, at], y_hbm.at[:, at], out_sem.at[i])

    for i in range(width // TILE):
        at = slice(i * TILE, (i + 1) * TILE)
        got = _dot(a_s[...], wo_s[:, at], 1, 0)
        x_s[:, at] = (x_s[:, at].astype(jnp.float32) + got).astype(jnp.bfloat16)
        out(i).start()
    for i in range(width // TILE):
        out(i).wait()


def _move(from_ref, to_ref, held, in_sem, out_sem):
    rows = from_ref.shape[0] // in_sem.shape[0]

    def take(i):
        at = pl.ds(i * rows, rows)
        return pltpu.make_async_copy(from_ref.at[at, :], held.at[at, :], in_sem.at[i])

    def give(i):
        at = pl.ds(i * rows, rows)
        return pltpu.make_async_copy(held.at[at, :], to_ref.at[at, :], out_sem.at[i])

    for i in range(in_sem.shape[0]):
        take(i).start()
    for i in range(in_sem.shape[0]):
        take(i).wait()
        give(i).start()
    for i in range(in_sem.shape[0]):
        give(i).wait()


def solution(mesh):
    n = mesh.shape["sp"]

    def step(x, gain, wq, wk, wv, wo):
        own, width = x.shape
        half = HEAD // 2
        rate = np.float64(THETA) ** (-np.arange(half) / half)
        angle = np.arange(own)[:, None] * rate
        start = (np.arange(n) * own)[:, None] * rate
        table = jnp.asarray(np.concatenate([np.cos(angle), np.sin(angle)], -1), jnp.float32)
        base = jnp.asarray(np.concatenate([np.cos(start), np.sin(start)], -1), jnp.float32)
        heads = wq.shape[1] // HEAD
        far = n // 4
        low, wide = jnp.bfloat16, jnp.float32
        dma = pltpu.SemaphoreType.DMA
        y = pl.pallas_call(
            functools.partial(_kernel, n),
            out_shape=jax.ShapeDtypeStruct(x.shape, x.dtype),
            in_specs=[pl.BlockSpec(memory_space=pl.ANY)] * 8,
            out_specs=pl.BlockSpec(memory_space=pl.ANY),
            scratch_shapes=[
                pltpu.VMEM((own, width), low), pltpu.VMEM((own, width), low), pltpu.VMEM((width,), low),
                pltpu.VMEM(wq.shape, low), pltpu.VMEM((width, 2 * HEAD), low), pltpu.VMEM(wo.shape, low),
                pltpu.VMEM((own, HEAD), wide), pltpu.VMEM((n, HEAD), wide),
                pltpu.VMEM((heads * own, HEAD), low), pltpu.VMEM((n, PARTS, own // PARTS + HEAD, HEAD), low),
                pltpu.VMEM((8, heads * own), wide), pltpu.VMEM((HEAD + 8, heads * own), wide),
                dma((6,)), dma((own // ROWS,)), dma((heads,)), dma((width // TILE,)), *[dma((far, PARTS))] * 4, *[dma((2 * far, PARTS))] * 2,
            ],
            compiler_params=pltpu.CompilerParams(collective_id=0, has_side_effects=True, vmem_limit_bytes=VMEM),
            cost_estimate=pl.CostEstimate(flops=60 * 10**9, bytes_accessed=24 * 2**20, transcendentals=0),
            name="layer",
        )(x, gain, wq, wk, wv, wo, table, base)
        return pl.pallas_call(
            _move,
            out_shape=jax.ShapeDtypeStruct(y.shape, y.dtype),
            in_specs=[pl.BlockSpec(memory_space=pl.ANY)],
            out_specs=pl.BlockSpec(memory_space=pl.ANY),
            scratch_shapes=[pltpu.VMEM(y.shape, y.dtype), dma((own // 64,)), dma((own // 64,))],
            compiler_params=pltpu.CompilerParams(vmem_limit_bytes=VMEM),
            cost_estimate=pl.CostEstimate(flops=2**30, bytes_accessed=4 * 2**20, transcendentals=0),
            name="move",
        )(y)

    tokens, whole = P(("dp", "sp"), None), P(None, None)
    return jax.shard_map(step, mesh=mesh, in_specs=(tokens, P(None), whole, whole, whole, whole), out_specs=tokens, check_vma=False)
```
